32 devices in a mesh: pipe: 4 (over y, x), dp: 2 (over core), expert: 4 (over z).
Axes of the slice: x: 2, y: 2, z: 4, core: 2. Of those that a mesh axis runs over, the one named last changes fastest.
Arguments:
- embedded: bfloat16 [1024, 2048], P(('dp', 'expert')), may hold values from -6 to 6
- section_out: bfloat16 [4, 1024, 2048], P('pipe', ('dp', 'expert')), may hold values from -6 to 6
- expert_ids: int32 [4, 1024, 6], P('pipe', ('dp', 'expert')), may hold values from 0 to 31, all different within a row
- route_weights: float32 [4, 1024, 6], P('pipe', ('dp', 'expert')), may hold values from 0.02 to 0.6
- valid_tokens: int32 [4, 8], P('pipe', ('dp', 'expert')), may hold values from 32 to 96, as said below
- w_gate_up: bfloat16 [4, 64, 2048, 704], P('pipe', 'expert'), may hold values from -0.125 to 0.125
- w_down: bfloat16 [4, 64, 352, 2048], P('pipe', 'expert'), may hold values from -0.21875 to 0.21875
Outputs:
- mixed: bfloat16 [4, 1024, 2048], P('pipe', ('dp', 'expert'))
- balance: float32 [4], P('pipe')
The draws below stay inside these ranges and needn't reach their ends.
Inputs may be any that keep to these rules, and one draw needn't show every extreme that they name: `expert_ids`: each row names 6 different experts. The first valid_tokens[s, g] rows of group g are real, the rest padding.
All inputs are finite; a program needn't handle non-finite values.
Results may differ from the reference program's by a relative error of at most 0.0027.
Values may be sent and summed in bfloat16 or wider, within the bound.
A program may use at most 128 MiB of HBM per device.

```python
import math
import jax
import jax.numpy as jnp
from jax import lax

D = 2048
FFE = 704
FF_DEV = 352
EXPERTS = 32
TOP = 6
CAP = 8
TOK_DEV = 128
EXP_DEV = 16
TOKENS = 1024
N_PIPE = 4
N_DP = 2
N_EXPERT = 4


def draw_valid_tokens(key, part):
    lower = TOK_DEV // 4
    upper = 3 * TOK_DEV // 4
    groups = N_DP * N_EXPERT
    order = jnp.arange(groups, dtype=jnp.int32)
    base = lower + order * (upper - lower) // max(groups - 1, 1)
    jitter = jax.random.randint(key, (N_PIPE, groups), 0, max((upper - lower) // 8, 1) + 1)
    jitter = jitter * (order < groups - 1).astype(jnp.int32)[None, :]
    return jnp.clip(base[None, :] - jitter, lower, upper).astype(jnp.int32)


def shard_levels(key, extent, split, least, top_value):
    factor_of, own = 1.0, jax.random.fold_in(key, 6)
    for dim, blocks in split:
        heights = jnp.exp(jax.random.uniform(jax.random.fold_in(own, dim), (blocks,), jnp.float32, least / len(split), top_value / len(split)))
        factor_of = factor_of * jnp.repeat(heights, extent[dim] // blocks).reshape([-1 if axis == dim else 1 for axis in range(len(extent))])
    return factor_of


def choose_distinct(own_key, rows, number_of, top, lift):
    order = jax.random.permutation(jax.random.fold_in(own_key, 1), number_of)
    boost = order
    for power in range(3):
        boost = boost * boost // number_of
    boost = boost * lift // number_of
    tickets = jax.random.randint(jax.random.fold_in(own_key, 2), (rows, number_of), 0, 4096) + boost
    holders = jax.random.permutation(jax.random.fold_in(own_key, 3), rows)[jnp.arange(number_of) % rows]
    tickets = jnp.where(jnp.arange(rows)[:, None] == holders[None, :], 1 << 14, tickets)
    priority = tickets * number_of + jnp.arange(number_of)
    return lax.top_k(priority.astype(jnp.int32), top)[1].astype(jnp.int32)


def scatter_about(own_key, extent, scale, limit, shards=(), held_as=jnp.bfloat16):
    entries = jax.random.normal(own_key, extent, jnp.float32) * scale
    if len(shards) > 0:
        entries = shard_levels(own_key, extent, shards, -0.22, 0.18) * entries
    return jnp.clip(entries, min=-limit, max=limit).astype(held_as)


def setup_inputs(seed: int = 0) -> dict:
    key_list = jax.random.split(jax.random.key(seed), 8)
    embedded = scatter_about(key_list[0], (TOKENS, D), 1.0, 6.0, ((0, 8),))
    section_out = scatter_about(key_list[1], (N_PIPE, TOKENS, D), 1.0, 6.0, ((0, 4), (1, 8)))
    expert_ids = choose_distinct(key_list[2], N_PIPE * TOKENS, EXPERTS, TOP, 3072).reshape((N_PIPE, TOKENS, TOP))
    route_weights = jnp.clip(jnp.exp(math.log(0.6) - 3.4011974 * jax.random.uniform(key_list[3], (N_PIPE, TOKENS, TOP), jnp.float32) ** shard_levels(key_list[3], (N_PIPE, TOKENS, TOP), ((0, 4), (1, 8)), -0.2, 0.2)), 0.02, 0.6)
    valid_tokens = draw_valid_tokens(jax.random.fold_in(key_list[7], 71), 0)
    w_gate_up = scatter_about(key_list[5], (N_PIPE, 2 * EXPERTS, D, 2 * FF_DEV), D ** -0.5, 0.125, ((0, 4), (1, 4)))
    w_down = scatter_about(key_list[6], (N_PIPE, 2 * EXPERTS, FF_DEV, D), FFE ** -0.5, 0.21875, ((0, 4), (1, 4)))
    return dict(embedded=embedded, section_out=section_out, expert_ids=expert_ids, route_weights=route_weights, valid_tokens=valid_tokens, w_gate_up=w_gate_up, w_down=w_down)


def route(expert_ids, route_weights, live_count):
    tok_count = expert_ids.shape[0]
    live_mask = (jnp.arange(tok_count, dtype=jnp.int32) < live_count)[:, None, None]
    chosen = ((expert_ids[:, :, None] == jnp.arange(EXPERTS, dtype=jnp.int32)[None, None, :]) & live_mask).astype(jnp.int32)
    flat_picks = chosen.reshape(tok_count * TOP, EXPERTS)
    earlier = jnp.cumsum(flat_picks, axis=0) - flat_picks
    slot_rank = jnp.sum(earlier * flat_picks, axis=1).reshape(tok_count, TOP)
    kept_mask = (jnp.sum(chosen, axis=2) > 0) & (slot_rank < CAP)
    slots = jnp.where(kept_mask, expert_ids * CAP + slot_rank, -1)
    counts = jnp.sum(flat_picks, axis=0).astype(jnp.float32)
    prob_sums = jnp.sum(chosen.astype(jnp.float32) * route_weights[:, :, None], axis=(0, 1))
    columns = jnp.arange(EXPERTS * CAP, dtype=jnp.int32)
    slot_hits = slots[:, :, None] == columns[None, None, :]
    dispatch = jnp.sum(slot_hits, axis=1).astype(jnp.float32)
    mixing = jnp.sum(jnp.where(slot_hits, route_weights[:, :, None], jnp.float32(0.0)), axis=1)
    return dispatch, mixing, counts, prob_sums


def expert_apply(operands):
    rows, w_in, w_out = operands
    parts = []
    for which in range(2):
        gate_up = jnp.dot(rows, w_in[which], preferred_element_type=jnp.float32)
        hidden = (jax.nn.silu(gate_up[:, :FF_DEV]) * gate_up[:, FF_DEV:]).astype(jnp.bfloat16)
        parts.append(jnp.dot(hidden, w_out[which], preferred_element_type=jnp.float32).astype(jnp.bfloat16))
    return (parts[0].astype(jnp.float32) + parts[1].astype(jnp.float32)).astype(jnp.bfloat16)


def reference(embedded, section_out, expert_ids, route_weights, valid_tokens, w_gate_up, w_down):
    groups = N_DP * N_EXPERT
    couples = N_EXPERT // 2
    outputs = []
    balances = []
    for section in range(N_PIPE):
        source = embedded if section == 0 else section_out[section - 1]
        incoming = source.reshape(groups, TOK_DEV, D)
        dispatch, mixing, counts, prob_sums = jax.vmap(route)(
            expert_ids[section].reshape(groups, TOK_DEV, TOP),
            route_weights[section].reshape(groups, TOK_DEV, TOP),
            valid_tokens[section])
        gathered = jnp.einsum('mts,mtd->msd', dispatch.astype(jnp.float32), incoming.astype(jnp.float32)).astype(jnp.bfloat16)
        per_expert = gathered.reshape(groups, EXPERTS, CAP, D).transpose(1, 0, 2, 3).reshape(EXPERTS, groups * CAP, D)
        w_in = w_gate_up[section].reshape(couples, 2, EXP_DEV, D, 2 * FF_DEV).transpose(0, 2, 1, 3, 4).reshape(EXPERTS, 2, D, 2 * FF_DEV)
        w_out = w_down[section].reshape(couples, 2, EXP_DEV, FF_DEV, D).transpose(0, 2, 1, 3, 4).reshape(EXPERTS, 2, FF_DEV, D)
        expert_rows = lax.map(expert_apply, (per_expert, w_in, w_out))
        merged = expert_rows.reshape(EXPERTS, groups, CAP, D).transpose(1, 0, 2, 3).reshape(groups, EXPERTS * CAP, D)
        branch = jnp.einsum('mts,msd->mtd', mixing, merged.astype(jnp.float32), precision=lax.Precision.HIGHEST)
        outputs.append((incoming.astype(jnp.float32) + branch).astype(jnp.bfloat16).reshape(TOKENS, D))
        live_total = jnp.sum(valid_tokens[section].astype(jnp.float32))
        total_counts = jnp.sum(counts, axis=0)
        total_probs = jnp.sum(prob_sums, axis=0)
        balances.append(EXPERTS * jnp.sum(total_counts * total_probs) / (TOP * live_total * live_total))
    return jnp.stack(outputs), jnp.stack(balances)
```

```python
import functools

import jax
import jax.numpy as jnp
from jax import lax
from jax.experimental import pallas as pl
from jax.experimental.pallas import tpu as pltpu
from jax.sharding import PartitionSpec as P

MESH = pl.DeviceIdType.MESH

EXPERTS = 32
TOP = 6
CAP = 8


def shifted(block, axis, distance):
    devices = range(lax.axis_size(axis))
    route = [(i - distance, i) for i in devices if i - distance in devices]
    return lax.ppermute(block, axis, route)


def route(expert_ids, route_weights, live_count):
    tok_count = expert_ids.shape[0]
    live_mask = (jnp.arange(tok_count, dtype=jnp.int32) < live_count)[:, None, None]
    chosen = (
        (expert_ids[:, :, None] == jnp.arange(EXPERTS, dtype=jnp.int32)[None, None, :]) & live_mask
    ).astype(jnp.int32)
    flat_picks = chosen.reshape(tok_count * TOP, EXPERTS)
    earlier = jnp.cumsum(flat_picks, axis=0) - flat_picks
    slot_rank = jnp.sum(earlier * flat_picks, axis=1).reshape(tok_count, TOP)
    kept_mask = (jnp.sum(chosen, axis=2) > 0) & (slot_rank < CAP)
    slots = jnp.where(kept_mask, expert_ids * CAP + slot_rank, -1)
    counts = jnp.sum(flat_picks, axis=0).astype(jnp.float32)
    prob_sums = jnp.sum(chosen.astype(jnp.float32) * route_weights[:, :, None], axis=(0, 1))
    columns = jnp.arange(EXPERTS * CAP, dtype=jnp.int32)
    slot_hits = slots[:, :, None] == columns[None, None, :]
    dispatch = jnp.sum(slot_hits, axis=1).astype(jnp.float32)
    mixing = jnp.sum(jnp.where(slot_hits, route_weights[:, :, None], jnp.float32(0.0)), axis=1)
    return (dispatch, mixing, counts, prob_sums)


def expert_ffn(tokens, w_in, w_out):
    gate_up = jnp.einsum("skcd,kdf->skcf", tokens, w_in, preferred_element_type=jnp.float32)
    hidden_width = w_out.shape[1]
    hidden = (jax.nn.silu(gate_up[..., :hidden_width]) * gate_up[..., hidden_width:]).astype(
        jnp.bfloat16
    )
    return jnp.einsum("skcf,kfd->skcd", hidden, w_out, preferred_element_type=jnp.float32).astype(
        jnp.bfloat16
    )


def on_device(embedded, section_out, expert_ids, route_weights, valid_tokens, w_gate_up, w_down):
    arrived = shifted(section_out[0], "pipe", 1)
    incoming = jnp.where(lax.axis_index("pipe") == 0, embedded, arrived)
    dispatch, mixing, counts, prob_sums = route(expert_ids[0], route_weights[0], valid_tokens[0, 0])
    live_total = valid_tokens[0, 0].astype(jnp.float32)
    totals = lax.psum((counts, prob_sums, live_total), ("dp", "expert"))
    gathered = jnp.einsum(
        "ts,td->sd", dispatch.astype(jnp.bfloat16), incoming, preferred_element_type=jnp.float32
    ).astype(jnp.bfloat16)
    devices = lax.axis_size("expert")
    couples = devices // 2
    local_count = w_gate_up.shape[1]
    model_width = incoming.shape[1]
    grouped = gathered.reshape(couples, local_count, CAP, model_width)
    weights_in = w_gate_up[0]
    weights_out = w_down[0]
    sent = jnp.broadcast_to(grouped[:, None], (couples, 2, local_count, CAP, model_width))
    sent = sent.reshape(devices, local_count * CAP, model_width)
    arrived_rows = lax.all_to_all(sent, "expert", split_axis=0, concat_axis=0, tiled=True).reshape(
        devices, local_count, CAP, model_width
    )
    partial_value = expert_ffn(arrived_rows, weights_in, weights_out)
    returned = lax.all_to_all(
        partial_value.reshape(devices, local_count * CAP, model_width),
        "expert",
        split_axis=0,
        concat_axis=0,
        tiled=True,
    )
    returned = returned.reshape(couples, 2, local_count, CAP, model_width)
    merged = (returned[:, 0].astype(jnp.float32) + returned[:, 1].astype(jnp.float32)).astype(
        jnp.bfloat16
    )
    merged = merged.reshape(EXPERTS * CAP, model_width)
    branch = jnp.dot(mixing, merged.astype(jnp.float32), precision=lax.Precision.HIGHEST)
    result = (incoming.astype(jnp.float32) + branch).astype(jnp.bfloat16)
    total_counts, total_probs, total_live = totals
    balance = EXPERTS * jnp.sum(total_counts * total_probs) / (TOP * total_live * total_live)
    return (result[None], balance.reshape(1))


STAGES = ((0, 1, 2, 3),)
WIDE = 512


def nearest(me, pos, count):
    found = 0
    for own in range(count):
        order = sorted(range(count), key=lambda other: (abs(other - own), other))
        found = found + jnp.where(me == own, order[pos], 0)
    return found


def relay_kernel(
    pipes, dps, line, live, rows,
    route_ref, embedded_ref, section_ref, w_in_ref, w_out_ref,
    mixed_ref, balance_ref,
    win, wout, tokens, tail, info, slots_in, slots_out, own_part, to_mate, from_mate,
    sent, from_left, from_right,
    w_sem, shift_send, own_recv, tail_sem, right_send, left_send, mate_send, mate_recv,
    info_send, info_recv, part_send, part_recv, back_send, left_recv, right_recv,
):
    p, d, y = lax.axis_index("pipe"), lax.axis_index("dp"), lax.axis_index("expert")
    mate = 1 - d
    tok_count, model_width = mixed_ref.shape
    half_count = win.shape[0]
    local_count = w_in_ref.shape[0]
    hidden_width = wout.shape[1]
    chunks = live // rows
    groups = dps * line
    experts = (line // 2) * local_count
    per_expert = dps * CAP
    slot_count = half_count * per_expert
    f32 = jnp.float32
    bf16 = jnp.bfloat16

    def w_copies(k):
        entry = d * half_count + k
        return (
            pltpu.make_async_copy(w_in_ref.at[entry], win.at[k], w_sem.at[0, k]),
            pltpu.make_async_copy(w_out_ref.at[entry], wout.at[k], w_sem.at[1, k]),
        )

    barrier = pltpu.get_barrier_semaphore()
    for g in range(1, groups):
        other = lax.rem(d * line + y + g, groups)
        pl.semaphore_signal(
            barrier, inc=1, device_id=(p, other // line, lax.rem(other, line)), device_id_type=MESH
        )

    @pl.when(p > 0)
    def _():
        pl.semaphore_signal(barrier, inc=1, device_id=(p - 1, d, y), device_id_type=MESH)

    @pl.when(p < pipes - 1)
    def _():
        pl.semaphore_signal(barrier, inc=1, device_id=(p + 1, d, y), device_id_type=MESH)

    def own_rows(c):
        return pl.ds(pl.multiple_of(d * tok_count + c * rows, rows), rows)

    def mate_rows(c):
        return pl.ds(pl.multiple_of(mate * tok_count + c * rows, rows), rows)

    tail_rows = tok_count - live

    def local_in(c):
        return pltpu.make_async_copy(
            embedded_ref.at[pl.ds(c * rows, rows)], tokens.at[y, own_rows(c)], own_recv.at[y, c]
        )

    local_tail = pltpu.make_async_copy(embedded_ref.at[pl.ds(live, tail_rows)], tail, tail_sem.at[1])

    @pl.when(p == 0)
    def _():
        for c in range(chunks):
            local_in(c).start()
        local_tail.start()

    ids = route_ref[0:8, :]
    expert_of = lax.broadcasted_iota(jnp.int32, (experts, tok_count), 0).astype(f32)
    hits = [(ids[k : k + 1, :] == expert_of).astype(f32) for k in range(TOP)]
    total = hits[0]
    for k in range(1, TOP):
        total = total + hits[k]
    before = (
        lax.broadcasted_iota(jnp.int32, (tok_count, tok_count), 0)
        < lax.broadcasted_iota(jnp.int32, (tok_count, tok_count), 1)
    ).astype(f32).astype(bf16)
    earlier = jnp.dot(total.astype(bf16), before, preferred_element_type=f32)
    me = d * line + y
    info[me, 0:8, :] = jnp.full((8, tok_count), -1.0, f32)
    for k in range(TOP):
        rank = jnp.sum(hits[k] * earlier, axis=0, keepdims=True)
        id_k = ids[k : k + 1, :]
        keep = (id_k >= 0.0) & (rank < CAP)
        code = id_k * per_expert + (d * CAP).astype(f32) + rank
        info[me, k : k + 1, :] = jnp.where(keep, code, -1.0)
    info[me, 8:24, :] = jnp.concatenate([route_ref[8:16, :], ids], axis=0)

    for z in range(line):
        for e in range(dps):
            lo = e * tok_count + live
            tokens[z, lo : lo + tail_rows, :] = jnp.zeros((tail_rows, model_width), bf16)

    pl.semaphore_wait(barrier, groups - 1 + (p > 0).astype(jnp.int32) + (p < pipes - 1).astype(jnp.int32))

    def shift(c):
        return pltpu.make_async_remote_copy(
            src_ref=section_ref.at[pl.ds(c * rows, rows)],
            dst_ref=tokens.at[y, own_rows(c)],
            send_sem=shift_send.at[c],
            recv_sem=own_recv.at[y, c],
            device_id=(p + 1, d, y),
            device_id_type=MESH,
        )

    shift_tail = pltpu.make_async_remote_copy(
        src_ref=section_ref.at[pl.ds(live, tail_rows)],
        dst_ref=tail,
        send_sem=tail_sem.at[0],
        recv_sem=tail_sem.at[1],
        device_id=(p + 1, d, y),
        device_id_type=MESH,
    )

    @pl.when(p < pipes - 1)
    def _():
        for c in range(chunks):
            shift(c).start()
        shift_tail.start()

    def info_copy(g):
        other = lax.rem(me + g, groups)
        return pltpu.make_async_remote_copy(
            src_ref=info.at[me],
            dst_ref=info.at[me],
            send_sem=info_send.at[g],
            recv_sem=info_recv.at[me],
            device_id=(p, other // line, lax.rem(other, line)),
            device_id_type=MESH,
        )

    for g in range(1, groups):
        info_copy(g).start()

    @pl.loop(0, half_count)
    def _(k):
        for copy in w_copies(k):
            copy.start()

    def along(z, c, send_sem, target):
        return pltpu.make_async_remote_copy(
            src_ref=tokens.at[z, own_rows(c)],
            dst_ref=tokens.at[z, own_rows(c)],
            send_sem=send_sem.at[z, c],
            recv_sem=own_recv.at[z, c],
            device_id=(p, d, target),
            device_id_type=MESH,
        )

    def across(z, c):
        return pltpu.make_async_remote_copy(
            src_ref=tokens.at[z, own_rows(c)],
            dst_ref=tokens.at[z, own_rows(c)],
            send_sem=mate_send.at[z, c],
            recv_sem=mate_recv.at[z, c],
            device_id=(p, mate, y),
            device_id_type=MESH,
        )

    def codes_of(e, z):
        return info[e * line + z]

    base = ((y // 2) * local_count + d * half_count) * per_expert

    def dispatch(pos):
        z = nearest(y, pos, line)
        code = jnp.concatenate([codes_of(e, z)[0:8, :] for e in range(dps)], axis=1) - base.astype(f32)
        slot_of = lax.broadcasted_iota(jnp.int32, (slot_count, dps * tok_count), 0).astype(f32)
        taken = (code[0:1, :] == slot_of).astype(f32)
        for k in range(1, TOP):
            taken = taken + (code[k : k + 1, :] == slot_of).astype(f32)
        taken = taken.astype(bf16)

        @pl.loop(0, model_width // WIDE)
        def _(n):
            cols = pl.ds(pl.multiple_of(n * WIDE, WIDE), WIDE)
            picked = jnp.dot(taken, tokens[z, :, cols], preferred_element_type=f32).astype(bf16)
            slots_in[pos, :, :, cols] = picked.reshape(half_count, per_expert, WIDE)

    def forward(pos, c):
        z = nearest(y, pos, line)
        pltpu.make_async_copy(tokens.at[z, own_rows(c)], tokens.at[z, own_rows(c)], own_recv.at[z, c]).wait()

        @pl.when((z <= y) & (y < line - 1))
        def _():
            along(z, c, right_send, y + 1).start()

        @pl.when((z >= y) & (y > 0))
        def _():
            along(z, c, left_send, y - 1).start()

        across(z, c).start()

    def mate_arrived(pos):
        z = nearest(y, pos, line)
        for c in range(chunks):
            pltpu.make_async_copy(
                tokens.at[z, mate_rows(c)], tokens.at[z, mate_rows(c)], mate_recv.at[z, c]
            ).wait()

    for pos in range(line):
        for c in range(chunks):
            forward(pos, c)
        if pos == 0:
            for g in range(1, groups):
                other = lax.rem(me + g, groups)
                pltpu.make_async_copy(info.at[other], info.at[other], info_recv.at[other]).wait()
        else:
            mate_arrived(pos - 1)
            dispatch(pos - 1)
    mate_arrived(line - 1)
    dispatch(line - 1)

    def against(x, columns):
        return lax.dot_general(x, columns, (((1,), (1,)), ((), ())), preferred_element_type=f32)

    for index, stage in enumerate(STAGES):
        first, last = stage[0], stage[-1] + 1
        count = (last - first) * per_expert

        @pl.loop(0, half_count)
        def _(k):
            if index == 0:
                for copy in w_copies(k):
                    copy.wait()
            x = slots_in[first:last, k].reshape(count, model_width)
            gate = against(x, win[k, :hidden_width])
            up = against(x, win[k, hidden_width:])
            hidden = (gate * (1.0 / (1.0 + jnp.exp(-gate))) * up).astype(bf16)

            @pl.loop(0, model_width // WIDE)
            def _(n):
                cols = pl.ds(pl.multiple_of(n * WIDE, WIDE), WIDE)
                out = jnp.dot(hidden, wout[k, :, cols], preferred_element_type=f32).astype(bf16)
                slots_out[first:last, k, :, cols] = out.reshape(last - first, per_expert, WIDE)

    def mix(pos, e, store):
        z = nearest(y, pos, line)
        record = info[e * line + z]
        code = record[0:8, :] - base.astype(f32)
        slot_of = lax.broadcasted_iota(jnp.int32, (slot_count, tok_count), 0).astype(f32)
        weights = jnp.zeros((slot_count, tok_count), f32)
        for k in range(TOP):
            weights = weights + jnp.where(code[k : k + 1, :] == slot_of, record[8 + k : 9 + k, :], 0.0)
        weights = weights.T
        high = weights.astype(bf16)
        low = (weights - high.astype(f32)).astype(bf16)

        @pl.loop(0, model_width // WIDE)
        def _(n):
            cols = pl.ds(pl.multiple_of(n * WIDE, WIDE), WIDE)
            values = slots_out[pos, :, :, cols].reshape(slot_count, WIDE)
            part = jnp.dot(high, values, preferred_element_type=f32) + jnp.dot(
                low, values, preferred_element_type=f32
            )
            store(cols, part[:live])

    def part_copy(pos):
        z = nearest(y, pos, line)
        return pltpu.make_async_remote_copy(
            src_ref=to_mate.at[z],
            dst_ref=from_mate.at[z],
            send_sem=part_send.at[z],
            recv_sem=part_recv.at[z],
            device_id=(p, mate, y),
            device_id_type=MESH,
        )

    def partials(pos):
        z = nearest(y, pos, line)

        def store_mate(cols, part):
            to_mate[z, :, cols] = part.astype(bf16)

        def store_own(cols, part):
            own_part[z, :, cols] = part

        mix(pos, mate, store_mate)
        part_copy(pos).start()
        mix(pos, d, store_own)

    def back(z, c, buffer, recv_sem, target):
        span = pl.ds(c * rows, rows)
        return pltpu.make_async_remote_copy(
            src_ref=sent.at[z, span],
            dst_ref=buffer.at[z, span],
            send_sem=back_send.at[z, c],
            recv_sem=recv_sem.at[z, c],
            device_id=(p, d, target),
            device_id_type=MESH,
        )

    def arrived(buffer, z, c, recv_sem):
        span = pl.ds(c * rows, rows)
        pltpu.make_async_copy(buffer.at[z, span], buffer.at[z, span], recv_sem.at[z, c]).wait()

    def pass_on(z, c, upstream, buffer, recv_sem, target):
        span = pl.ds(c * rows, rows)

        @pl.when(upstream)
        def _():
            arrived(buffer, z, c, recv_sem)
            sent[z, span] = (
                own_part[z, span] + from_mate[z, span].astype(f32) + buffer[z, span].astype(f32)
            ).astype(bf16)

        @pl.when(jnp.logical_not(upstream))
        def _():
            sent[z, span] = (own_part[z, span] + from_mate[z, span].astype(f32)).astype(bf16)

        back(z, c, buffer, recv_sem, target).start()

    def chain(pos):
        z = nearest(y, pos, line)
        part_copy(pos).wait_recv()

        @pl.when(z > y)
        def _():
            for c in range(chunks):
                pass_on(z, c, y > 0, from_left, left_recv, y + 1)

        @pl.when(z < y)
        def _():
            for c in range(chunks):
                pass_on(z, c, y < line - 1, from_right, right_recv, y - 1)

    for pos in range(line - 1, -1, -1):
        partials(pos)
        if pos < line - 1:
            chain(pos + 1)

    counts = jnp.zeros((experts, tok_count), f32)
    probs = jnp.zeros((experts, tok_count), f32)
    real = jnp.zeros((1, tok_count), f32)
    for g in range(groups):
        record = info[g]
        for k in range(TOP):
            hit = record[16 + k : 17 + k, :] == expert_of
            counts = counts + hit.astype(f32)
            probs = probs + jnp.where(hit, record[8 + k : 9 + k, :], 0.0)
        real = real + (record[16:17, :] >= 0.0).astype(f32)
    by_expert = jnp.sum(counts, axis=1, keepdims=True) * jnp.sum(probs, axis=1, keepdims=True)
    live_total = jnp.sum(real, axis=1, keepdims=True)
    balance = experts * jnp.sum(by_expert, axis=0, keepdims=True) / (TOP * live_total * live_total)
    balance_ref[...] = jnp.broadcast_to(balance, balance_ref.shape)

    part_copy(0).wait_recv()

    @pl.when(p < pipes - 1)
    def _():
        shift_tail.wait_send()

    pltpu.make_async_copy(tail, tail, tail_sem.at[1]).wait()
    mixed_ref[live:, :] = tail[...]
    for c in range(chunks):
        span = pl.ds(c * rows, rows)
        own_part[y, span] = (
            own_part[y, span]
            + from_mate[y, span].astype(f32)
            + tokens[y, own_rows(c), :].astype(f32)
        )

        @pl.when(y > 0)
        def _():
            arrived(from_left, y, c, left_recv)
            own_part[y, span] = own_part[y, span] + from_left[y, span].astype(f32)

        @pl.when(y < line - 1)
        def _():
            arrived(from_right, y, c, right_recv)
            own_part[y, span] = own_part[y, span] + from_right[y, span].astype(f32)

        mixed_ref[span, :] = own_part[y, span].astype(bf16)

    for g in range(1, groups):
        info_copy(g).wait_send()

    @pl.when(p < pipes - 1)
    def _():
        for c in range(chunks):
            shift(c).wait_send()

    for pos in range(line):
        z = nearest(y, pos, line)
        part_copy(pos).wait_send()
        for c in range(chunks):
            across(z, c).wait_send()

            @pl.when((z <= y) & (y < line - 1))
            def _():
                along(z, c, right_send, y + 1).wait_send()

            @pl.when((z >= y) & (y > 0))
            def _():
                along(z, c, left_send, y - 1).wait_send()

            if pos > 0:
                back(z, c, from_left, left_recv, y).wait_send()


def fused(sizes, embedded, section_out, expert_ids, route_weights, valid_tokens, w_gate_up, w_down):
    pipes, dps, line = sizes["pipe"], sizes["dp"], sizes["expert"]
    tok_count, model_width = embedded.shape
    local_count, _, both_width = w_gate_up.shape[1:]
    hidden_width = w_down.shape[2]
    half_count = local_count // dps
    live = tok_count * 3 // 4
    rows = 32
    chunks = live // rows
    groups = dps * line
    per_expert = dps * CAP
    live_row = jnp.arange(tok_count, dtype=jnp.int32)[None, :] < valid_tokens[0, 0]
    ids = jnp.where(live_row, expert_ids[0].T, -1).astype(jnp.float32)
    pad = ((0, 8 - TOP), (0, 0))
    route_in = jnp.concatenate(
        [jnp.pad(ids, pad, constant_values=-1.0), jnp.pad(route_weights[0].T, pad)], axis=0
    )
    bf16, f32 = jnp.bfloat16, jnp.float32
    dma = pltpu.SemaphoreType.DMA
    vmem = pl.BlockSpec(memory_space=pltpu.VMEM)
    hbm = pl.BlockSpec(memory_space=pl.ANY)
    mixed, balance = pl.pallas_call(
        functools.partial(relay_kernel, pipes, dps, line, live, rows),
        out_shape=(
            jax.ShapeDtypeStruct((tok_count, model_width), bf16),
            jax.ShapeDtypeStruct((8, 128), f32),
        ),
        in_specs=[vmem, hbm, hbm, hbm, hbm],
        out_specs=(vmem, vmem),
        scratch_shapes=[
            pltpu.VMEM((half_count, both_width, model_width), bf16),
            pltpu.VMEM((half_count, hidden_width, model_width), bf16),
            pltpu.VMEM((line, dps * tok_count, model_width), bf16),
            pltpu.VMEM((tok_count - live, model_width), bf16),
            pltpu.VMEM((groups, 24, tok_count), f32),
            pltpu.VMEM((line, half_count, per_expert, model_width), bf16),
            pltpu.VMEM((line, half_count, per_expert, model_width), bf16),
            pltpu.VMEM((line, live, model_width), f32),
            pltpu.VMEM((line, live, model_width), bf16),
            pltpu.VMEM((line, live, model_width), bf16),
            pltpu.VMEM((line, live, model_width), bf16),
            pltpu.VMEM((line, live, model_width), bf16),
            pltpu.VMEM((line, live, model_width), bf16),
            dma((2, half_count)),
            dma((chunks,)),
            dma((line, chunks)),
            dma((2,)),
            dma((line, chunks)),
            dma((line, chunks)),
            dma((line, chunks)),
            dma((line, chunks)),
            dma((groups,)),
            dma((groups,)),
            dma((line,)),
            dma((line,)),
            dma((line, chunks)),
            dma((line, chunks)),
            dma((line, chunks)),
        ],
        compiler_params=pltpu.CompilerParams(
            collective_id=0, has_side_effects=True, vmem_limit_bytes=67043328
        ),
    )(route_in, embedded, section_out[0], jnp.swapaxes(w_gate_up[0], 1, 2), w_down[0])
    return mixed[None], balance[0, :1]


def step(sizes, *args):
    local_count = args[5].shape[1]
    if sizes["dp"] == 2 and sizes["expert"] == 4 and local_count % 2 == 0:
        return fused(sizes, *args)
    return on_device(*args)


def solution(mesh):
    return jax.shard_map(
        functools.partial(step, dict(mesh.shape)),
        mesh=mesh,
        in_specs=(
            P(("dp", "expert"), None),
            P("pipe", ("dp", "expert"), None),
            P("pipe", ("dp", "expert"), None),
            P("pipe", ("dp", "expert"), None),
            P("pipe", ("dp", "expert")),
            P("pipe", "expert", None, None),
            P("pipe", "expert", None, None),
        ),
        out_specs=(P("pipe", ("dp", "expert"), None), P("pipe")),
        check_vma=False,
    )
```
